32 devices in a mesh: expert: 16 (over z, y, core), tensor: 2 (over x).
Axes of the slice: x: 2, y: 2, z: 4, core: 2. Of those that a mesh axis runs over, the one named last changes fastest.
Arguments:
- tokens: bfloat16 [64, 256, 1280], P(('expert', 'tensor')), may hold values from -6 to 6
- slot_keys: bfloat16 [1280, 16], replicated, may hold values from -6 to 6
- logit_scale: float32 [], replicated, may hold values from 40 to 80
- w_in: bfloat16 [16, 1280, 3584], P('expert', None, 'tensor'), may hold values from -0.625 to 0.625
- b_in: bfloat16 [16, 3584], P('expert', 'tensor'), may hold values from -3 to 3
- w_out: bfloat16 [16, 3584, 1280], P('expert', 'tensor'), may hold values from -0.09375 to 0.09375
- b_out: bfloat16 [16, 1280], P('expert'), may hold values from -3 to 3
Outputs:
- mixed: bfloat16 [64, 256, 1280], P(('expert', 'tensor'))
The draws below stay inside these ranges and needn't reach their ends.
All inputs are finite; a program needn't handle non-finite values.
Results may differ from the reference program's by a relative error of at most 0.0071.
Values may be sent and summed in bfloat16 or wider, within the bound.
A program may use at most 64 MiB of HBM per device.

```python
import math
import jax
import jax.numpy as jnp
from jax import lax

D = 1280
FF = 3584
SEQ = 256
EXPERTS = 16
IMAGES = 64


def shard_levels(key, shape, split, smallest, top_value):
    factor_of, own = 1.0, jax.random.fold_in(key, 6)
    for position, shards_of in split:
        heights = jnp.exp(jax.random.uniform(jax.random.fold_in(own, position), (shards_of,), jnp.float32, smallest / len(split), top_value / len(split)))
        factor_of = factor_of * jnp.repeat(heights, shape[position] // shards_of).reshape([-1 if axis == position else 1 for axis in range(len(shape))])
    return factor_of


def noise(own_key, dims, width, limit, pieces=(), held_as=jnp.bfloat16):
    values = width * jax.random.normal(own_key, dims, jnp.float32)
    if pieces:
        values = values * shard_levels(own_key, dims, pieces, -0.22, 0.18)
    return jnp.clip(values, -limit, limit).astype(held_as)


def setup_inputs(seed: int = 0) -> dict:
    streams_of = jax.random.split(jax.random.key(seed), 8)
    tokens = noise(streams_of[0], (IMAGES, SEQ, D), 1.0, 6.0, ((0, 32),))
    slot_keys = noise(streams_of[1], (D, EXPERTS), 1.0, 6.0)
    logit_scale = jnp.clip(jnp.exp(jax.random.uniform(streams_of[2], (), jnp.float32, math.log(40.0), math.log(80.0))), 40.0, 80.0)
    w_in = noise(streams_of[3], (EXPERTS, D, FF), (D // 16) ** -0.5, 0.625, ((0, 16), (2, 2)))
    b_in = noise(streams_of[4], (EXPERTS, FF), 0.5, 3.0, ((0, 16), (1, 2)))
    w_out = noise(streams_of[5], (EXPERTS, FF, D), FF ** -0.5, 0.09375, ((0, 16), (1, 2)))
    b_out = noise(streams_of[6], (EXPERTS, D), 0.5, 3.0, ((0, 16),))
    return {"tokens": tokens, "slot_keys": slot_keys, "logit_scale": logit_scale, "w_in": w_in, "b_in": b_in, "w_out": w_out, "b_out": b_out}


EPS = 1e-06

def expert_apply(args):
    slot_rows, weight_in, bias_in, weight_out, bias_out = args
    pre = jnp.dot(slot_rows, weight_in, preferred_element_type=jnp.float32) + bias_in.astype(jnp.float32)
    hidden = jax.nn.gelu(pre).astype(jnp.bfloat16)
    result = jnp.dot(hidden, weight_out, preferred_element_type=jnp.float32) + bias_out.astype(jnp.float32)
    return result.astype(jnp.bfloat16)

def reference(tokens, slot_keys, logit_scale, w_in, b_in, w_out, b_out):
    tok_wide = tokens.astype(jnp.float32)
    key_wide = slot_keys.astype(jnp.float32)
    row_inv = lax.rsqrt(lax.optimization_barrier(jnp.sum(tok_wide * tok_wide, axis=2, keepdims=True)) + EPS)
    key_inv = lax.rsqrt(lax.optimization_barrier(jnp.sum(key_wide * key_wide, axis=0)) + EPS)
    raw = jnp.einsum('imd,ds->ims', tok_wide, key_wide)
    logits = logit_scale * row_inv * key_inv * raw
    expo = jnp.exp(logits)
    dispatch = (expo / lax.optimization_barrier(jnp.sum(expo, axis=1, keepdims=True))).astype(jnp.bfloat16)
    combine = (expo / lax.optimization_barrier(jnp.sum(expo, axis=2, keepdims=True))).astype(jnp.bfloat16)
    slot_in = jnp.einsum('ims,imd->sid', dispatch.astype(jnp.float32), tok_wide).astype(jnp.bfloat16)
    slot_out = lax.map(expert_apply, (slot_in, w_in, b_in, w_out, b_out))
    mixed = jnp.einsum('ims,sid->imd', combine.astype(jnp.float32), slot_out.astype(jnp.float32))
    return mixed.astype(jnp.bfloat16)
```

```python
import functools

import jax
import jax.numpy as jnp
from jax import lax
from jax.experimental import pallas as pl
from jax.experimental.pallas import tpu as pltpu
from jax.sharding import PartitionSpec as P

EPS = 1e-06
LOGICAL = pl.DeviceIdType.LOGICAL
NT = (((1,), (1,)), ((), ()))
UNROLL = 64
TILE = 256
SPLIT = 2


def peers_of(mesh):
    flat = list(mesh.devices.flat)
    devices = len(flat)

    def hops(k):
        a, b = (getattr(d, "coords", (0, 0, 0)) for d in (flat[0], flat[k]))
        return sum(abs(p - q) for p, q in zip(a, b))

    return sorted(range(1, devices), key=lambda k: (-hops(k), -k))


def kernel(
    experts, tensors, steps,
    tokens_hbm, keys_hbm, scale_hbm, w_in_hbm, b_in_hbm, w_out_hbm, b_out_hbm,
    recv2, comb,
    tok, keys_ref, scale_ref, b_in_ref, b_out_ref, w_in, w_out, send1, recv1, hidden, send2,
    load_sem, send_sem1, recv_sem1, send_sem2, recv_sem2,
):
    images, seq, width = tok.shape
    slots = keys_ref.shape[0]
    rows = slots * images
    devices = experts * tensors
    e, t = lax.axis_index("expert"), lax.axis_index("tensor")
    me = e * tensors + t
    home = t * experts + e
    pow2 = devices & (devices - 1) == 0

    def each_peer(body):
        if pow2 and devices <= UNROLL:
            for k in steps:
                body(me ^ k)
        else:
            @pl.loop(1, devices)
            def _(step):
                body(lax.rem(me + step, devices))

    barrier = pltpu.get_barrier_semaphore()
    each_peer(lambda j: pl.semaphore_signal(barrier, inc=1, device_id=j, device_id_type=LOGICAL))

    pairs = [
        (keys_hbm, keys_ref), (scale_hbm, scale_ref), (tokens_hbm, tok), (b_in_hbm, b_in_ref),
        (w_in_hbm.at[0], w_in), (b_out_hbm, b_out_ref), (w_out_hbm.at[0], w_out),
    ]
    loads = [pltpu.make_async_copy(src, dst, load_sem.at[i]) for i, (src, dst) in enumerate(pairs)]
    for load in loads:
        load.start()

    loads[0].wait()
    loads[1].wait()
    row_slot = lax.broadcasted_iota(jnp.int32, (rows, slots), 0) // images
    col_slot = lax.broadcasted_iota(jnp.int32, (rows, slots), 1)
    spread = jnp.where(row_slot == col_slot, 1.0, 0.0).astype(jnp.bfloat16)
    keys_t = jnp.dot(spread, keys_ref[...], preferred_element_type=jnp.float32)
    key_inv = lax.rsqrt(jnp.sum(keys_t * keys_t, axis=1, keepdims=True) + EPS)
    key_gain = key_inv * scale_ref[0]
    keys_b = keys_t.astype(jnp.bfloat16)

    loads[2].wait()
    flat = tok[...].reshape(images * seq, width)
    raw = lax.dot_general(keys_b, flat, NT, preferred_element_type=jnp.float32)
    part = jnp.zeros((images * seq, 128), jnp.float32)
    for c in range(width // 128):
        piece = flat[:, c * 128:(c + 1) * 128].astype(jnp.float32)
        part = part + piece * piece
    row_sq = lax.dot_general(
        jnp.ones((8, 128), jnp.float32), part, NT,
        precision=lax.Precision.HIGHEST, preferred_element_type=jnp.float32,
    )[0:1]
    logits = key_gain * lax.rsqrt(row_sq + EPS) * raw
    row_image = lax.broadcasted_iota(jnp.int32, logits.shape, 0) % images
    col_image = lax.broadcasted_iota(jnp.int32, logits.shape, 1) // seq
    expo = jnp.where(row_image == col_image, jnp.exp(logits), 0.0)
    dispatch = (expo / jnp.sum(expo, axis=1, keepdims=True)).astype(jnp.bfloat16)
    slot_in = jnp.dot(dispatch, flat, preferred_element_type=jnp.float32).astype(jnp.bfloat16)
    for s in range(slots):
        send1[s] = slot_in[s * images:(s + 1) * images]
    recv1[me] = send1[e]
    combine = expo / jnp.sum(expo, axis=0, keepdims=True)
    comb[...] = jnp.concatenate([combine] * tensors, axis=0).T.astype(jnp.bfloat16)

    pl.semaphore_wait(barrier, devices - 1)
    each_peer(lambda j: pltpu.make_async_remote_copy(
        src_ref=send1.at[j // tensors], dst_ref=recv1.at[me], send_sem=send_sem1, recv_sem=recv_sem1,
        device_id=j, device_id_type=LOGICAL,
    ).start())

    for load in loads[3:]:
        load.wait()
    others = recv1.at[pl.ds(0, devices - 1)]
    pltpu.make_async_copy(others, others, recv_sem1).wait()
    x = recv1[...].reshape(devices * images, width)
    half = w_in.shape[1]
    first_half = jnp.where(t == 0, 1.0, 0.0)
    for c in range(0, half, TILE):
        size = min(TILE, half - c)
        pre = jnp.dot(x, w_in[:, c:c + size], preferred_element_type=jnp.float32)
        pre = pre + b_in_ref[:, c:c + size].astype(jnp.float32)
        hidden[:, c:c + size] = jax.nn.gelu(pre).astype(jnp.bfloat16)
    y = jnp.dot(hidden[...], w_out[...], preferred_element_type=jnp.float32)
    y = y + b_out_ref[...].astype(jnp.float32) * first_half
    send2[...] = y.astype(jnp.bfloat16).reshape(devices, images, width)
    recv2[home] = send2[me]
    each_peer(lambda j: pltpu.make_async_remote_copy(
        src_ref=send2.at[j], dst_ref=recv2.at[home], send_sem=send_sem2, recv_sem=recv_sem2,
        device_id=j, device_id_type=LOGICAL,
    ).start())

    pltpu.make_async_copy(others, others, send_sem1).wait()
    block = recv2.at[pl.ds(0, devices - 1)]
    pltpu.make_async_copy(block, block, send_sem2).wait()
    pltpu.make_async_copy(block, block, recv_sem2).wait()


def mix(chunk, recv2, comb, out_hbm, out, sem):
    images, seq, width = out_hbm.shape
    r = recv2[...].reshape(-1, width)
    copies = []
    for c in range(images * seq // chunk):
        mixed = jnp.dot(comb[c * chunk:(c + 1) * chunk], r, preferred_element_type=jnp.float32)
        at = (c * chunk // seq, pl.ds(c * chunk % seq, chunk))
        out[at[0], at[1]] = mixed.astype(jnp.bfloat16)
        copies.append(pltpu.make_async_copy(out.at[at[0], at[1]], out_hbm.at[at[0], at[1]], sem.at[c]))
        copies[-1].start()
    for copy in copies:
        copy.wait()


def local(experts, tensors, steps, tokens, slot_keys, logit_scale, w_in, b_in, w_out, b_out):
    images, seq, width = tokens.shape
    slots = slot_keys.shape[1]
    half = w_in.shape[2]
    devices = experts * tensors
    bf16 = jnp.bfloat16
    recv2, comb = pl.pallas_call(
        functools.partial(kernel, experts, tensors, steps),
        out_shape=[
            pltpu.VMEM((devices, images, width), bf16),
            pltpu.VMEM((images * seq, tensors * slots * images), bf16),
        ],
        in_specs=[pl.BlockSpec(memory_space=pltpu.HBM)] * 7,
        out_specs=[pl.BlockSpec(memory_space=pltpu.VMEM)] * 2,
        scratch_shapes=[
            pltpu.VMEM((images, seq, width), bf16),
            pltpu.VMEM((slots, width), bf16),
            pltpu.SMEM((1,), jnp.float32),
            pltpu.VMEM((1, half), bf16),
            pltpu.VMEM((1, width), bf16),
            pltpu.VMEM((width, half), bf16),
            pltpu.VMEM((half, width), bf16),
            pltpu.VMEM((slots, images, width), bf16),
            pltpu.VMEM((devices, images, width), bf16),
            pltpu.VMEM((devices * images, half), bf16),
            pltpu.VMEM((devices, images, width), bf16),
            pltpu.SemaphoreType.DMA((7,)),
            pltpu.SemaphoreType.DMA,
            pltpu.SemaphoreType.DMA,
            pltpu.SemaphoreType.DMA,
            pltpu.SemaphoreType.DMA,
        ],
        compiler_params=pltpu.CompilerParams(collective_id=0, has_side_effects=True, vmem_limit_bytes=55 * 2**20),
    )(tokens, slot_keys.T, logit_scale.reshape(1), w_in, b_in, w_out, b_out)
    chunk = seq // SPLIT
    return pl.pallas_call(
        functools.partial(mix, chunk),
        out_shape=jax.ShapeDtypeStruct(tokens.shape, bf16),
        in_specs=[pl.BlockSpec(memory_space=pltpu.VMEM)] * 2,
        out_specs=pl.BlockSpec(memory_space=pltpu.HBM),
        scratch_shapes=[
            pltpu.VMEM(tokens.shape, bf16),
            pltpu.SemaphoreType.DMA((images * seq // chunk,)),
        ],
        compiler_params=pltpu.CompilerParams(vmem_limit_bytes=16 * 2**20),
    )(recv2, comb)


def solution(mesh):
    placed = (
        P(("expert", "tensor"), None, None),
        P(),
        P(),
        P("expert", None, "tensor"),
        P("expert", "tensor"),
        P("expert", "tensor", None),
        P("expert", None),
    )
    return jax.shard_map(
        functools.partial(local, mesh.shape["expert"], mesh.shape["tensor"], peers_of(mesh)),
        mesh=mesh,
        in_specs=placed,
        out_specs=P(("expert", "tensor"), None, None),
        check_vma=False,
    )
```

```python
import functools

import jax
import jax.numpy as jnp
from jax import lax
from jax.experimental import pallas as pl
from jax.experimental.pallas import tpu as pltpu
from jax.sharding import PartitionSpec as P

EPS = 1e-06
LOGICAL = pl.DeviceIdType.LOGICAL
NT = (((1,), (1,)), ((), ()))
UNROLL = 64
TILE = 256
SPLIT = 2


def peers_of(mesh):
    flat = list(mesh.devices.flat)
    where = [tuple(getattr(d, "coords", None) or (0, 0, 0)) for d in flat]
    away = [[abs(p - q) for p, q in zip(w, where[0])] for w in where]
    axis = max(range(len(where[0])), key=lambda a: max(w[a] for w in away))
    groups = {}
    for k in sorted(range(1, len(flat)), key=lambda k: (-sum(away[k]), -k)):
        groups.setdefault(away[k][axis], []).append(k)
    steps = []
    while any(groups.values()):
        for g in sorted(groups, reverse=True):
            steps += groups[g][:1]
            del groups[g][:1]
    first = [k for k in range(len(flat)) if where[k] == where[0]][:2]
    return steps, first


def kernel(
    experts, tensors, order,
    tokens_hbm, keys_hbm, scale_hbm, w_in_hbm, b_in_hbm, w_out_hbm, b_out_hbm,
    recv2, comb,
    tok, keys_ref, scale_ref, b_in_ref, b_out_ref, w_in, w_out, send1, recv1, hidden, send2,
    load_sem, send_sem1, recv_sem1, send_sem2, recv_sem2,
):
    images, seq, width = tok.shape
    slots = keys_ref.shape[0]
    rows = slots * images
    devices = experts * tensors
    e, t = lax.axis_index("expert"), lax.axis_index("tensor")
    me = e * tensors + t
    home = t * experts + e
    steps, first = order
    pow2 = devices & (devices - 1) == 0

    def each_peer(body, ahead=()):
        if pow2 and devices <= UNROLL:
            for j in ahead:
                pl.when(me != j)(functools.partial(body, j))
            for k in steps:
                j = me ^ k
                if ahead:
                    rest = functools.reduce(jnp.logical_and, [j != a for a in ahead])
                    pl.when(rest)(functools.partial(body, j))
                else:
                    body(j)
        else:
            @pl.loop(1, devices)
            def _(step):
                body(lax.rem(me + step, devices))

    barrier = pltpu.get_barrier_semaphore()
    each_peer(lambda j: pl.semaphore_signal(barrier, inc=1, device_id=j, device_id_type=LOGICAL))

    pairs = [
        (keys_hbm, keys_ref), (scale_hbm, scale_ref), (tokens_hbm, tok), (b_in_hbm, b_in_ref),
        (w_in_hbm.at[0], w_in), (b_out_hbm, b_out_ref), (w_out_hbm.at[0], w_out),
    ]
    loads = [pltpu.make_async_copy(src, dst, load_sem.at[i]) for i, (src, dst) in enumerate(pairs)]
    for load in loads:
        load.start()

    loads[0].wait()
    loads[1].wait()
    row_slot = lax.broadcasted_iota(jnp.int32, (rows, slots), 0) // images
    col_slot = lax.broadcasted_iota(jnp.int32, (rows, slots), 1)
    spread = jnp.where(row_slot == col_slot, 1.0, 0.0).astype(jnp.bfloat16)
    keys_t = jnp.dot(spread, keys_ref[...], preferred_element_type=jnp.float32)
    key_inv = lax.rsqrt(jnp.sum(keys_t * keys_t, axis=1, keepdims=True) + EPS)
    key_gain = key_inv * scale_ref[0]
    keys_b = keys_t.astype(jnp.bfloat16)

    loads[2].wait()
    flat = tok[...].reshape(images * seq, width)
    raw = lax.dot_general(keys_b, flat, NT, preferred_element_type=jnp.float32)
    part = jnp.zeros((images * seq, 128), jnp.float32)
    for c in range(width // 128):
        piece = flat[:, c * 128:(c + 1) * 128].astype(jnp.float32)
        part = part + piece * piece
    row_sq = lax.dot_general(
        jnp.ones((8, 128), jnp.float32), part, NT,
        precision=lax.Precision.HIGHEST, preferred_element_type=jnp.float32,
    )[0:1]
    logits = key_gain * lax.rsqrt(row_sq + EPS) * raw
    row_image = lax.broadcasted_iota(jnp.int32, logits.shape, 0) % images
    col_image = lax.broadcasted_iota(jnp.int32, logits.shape, 1) // seq
    expo = jnp.where(row_image == col_image, jnp.exp(logits), 0.0)
    dispatch = (expo / jnp.sum(expo, axis=1, keepdims=True)).astype(jnp.bfloat16)
    slot_in = jnp.dot(dispatch, flat, preferred_element_type=jnp.float32).astype(jnp.bfloat16)
    for s in range(slots):
        send1[s] = slot_in[s * images:(s + 1) * images]
    recv1[me] = send1[e]
    combine = expo / jnp.sum(expo, axis=0, keepdims=True)
    comb[...] = jnp.concatenate([combine] * tensors, axis=0).T.astype(jnp.bfloat16)

    pl.semaphore_wait(barrier, devices - 1)
    each_peer(lambda j: pltpu.make_async_remote_copy(
        src_ref=send1.at[j // tensors], dst_ref=recv1.at[me], send_sem=send_sem1, recv_sem=recv_sem1,
        device_id=j, device_id_type=LOGICAL,
    ).start())

    for load in loads[3:]:
        load.wait()
    others = recv1.at[pl.ds(0, devices - 1)]
    pltpu.make_async_copy(others, others, recv_sem1).wait()
    x = recv1[...].reshape(devices * images, width)
    half = w_in.shape[1]
    first_half = jnp.where(t == 0, 1.0, 0.0)
    for c in range(0, half, TILE):
        size = min(TILE, half - c)
        pre = jnp.dot(x, w_in[:, c:c + size], preferred_element_type=jnp.float32)
        pre = pre + b_in_ref[:, c:c + size].astype(jnp.float32)
        hidden[:, c:c + size] = jax.nn.gelu(pre).astype(jnp.bfloat16)
    y = jnp.dot(hidden[...], w_out[...], preferred_element_type=jnp.float32)
    y = y + b_out_ref[...].astype(jnp.float32) * first_half
    send2[...] = y.astype(jnp.bfloat16).reshape(devices, images, width)
    recv2[home] = send2[me]
    each_peer(lambda j: pltpu.make_async_remote_copy(
        src_ref=send2.at[j], dst_ref=recv2.at[home], send_sem=send_sem2, recv_sem=recv_sem2,
        device_id=j, device_id_type=LOGICAL,
    ).start(), first)

    pltpu.make_async_copy(others, others, send_sem1).wait()
    block = recv2.at[pl.ds(0, devices - 1)]
    pltpu.make_async_copy(block, block, send_sem2).wait()
    pltpu.make_async_copy(block, block, recv_sem2).wait()


def mix(chunk, recv2, comb, out_hbm, out, sem):
    images, seq, width = out_hbm.shape
    r = recv2[...].reshape(-1, width)
    copies = []
    for c in range(images * seq // chunk):
        mixed = jnp.dot(comb[c * chunk:(c + 1) * chunk], r, preferred_element_type=jnp.float32)
        at = (c * chunk // seq, pl.ds(c * chunk % seq, chunk))
        out[at[0], at[1]] = mixed.astype(jnp.bfloat16)
        copies.append(pltpu.make_async_copy(out.at[at[0], at[1]], out_hbm.at[at[0], at[1]], sem.at[c]))
        copies[-1].start()
    for copy in copies:
        copy.wait()


def local(experts, tensors, order, tokens, slot_keys, logit_scale, w_in, b_in, w_out, b_out):
    images, seq, width = tokens.shape
    slots = slot_keys.shape[1]
    half = w_in.shape[2]
    devices = experts * tensors
    bf16 = jnp.bfloat16
    recv2, comb = pl.pallas_call(
        functools.partial(kernel, experts, tensors, order),
        out_shape=[
            pltpu.VMEM((devices, images, width), bf16),
            pltpu.VMEM((images * seq, tensors * slots * images), bf16),
        ],
        in_specs=[pl.BlockSpec(memory_space=pltpu.HBM)] * 7,
        out_specs=[pl.BlockSpec(memory_space=pltpu.VMEM)] * 2,
        scratch_shapes=[
            pltpu.VMEM((images, seq, width), bf16),
            pltpu.VMEM((slots, width), bf16),
            pltpu.SMEM((1,), jnp.float32),
            pltpu.VMEM((1, half), bf16),
            pltpu.VMEM((1, width), bf16),
            pltpu.VMEM((width, half), bf16),
            pltpu.VMEM((half, width), bf16),
            pltpu.VMEM((slots, images, width), bf16),
            pltpu.VMEM((devices, images, width), bf16),
            pltpu.VMEM((devices * images, half), bf16),
            pltpu.VMEM((devices, images, width), bf16),
            pltpu.SemaphoreType.DMA((7,)),
            pltpu.SemaphoreType.DMA,
            pltpu.SemaphoreType.DMA,
            pltpu.SemaphoreType.DMA,
            pltpu.SemaphoreType.DMA,
        ],
        compiler_params=pltpu.CompilerParams(collective_id=0, has_side_effects=True, vmem_limit_bytes=55 * 2**20),
    )(tokens, slot_keys.T, logit_scale.reshape(1), w_in, b_in, w_out, b_out)
    chunk = seq // SPLIT
    return pl.pallas_call(
        functools.partial(mix, chunk),
        out_shape=jax.ShapeDtypeStruct(tokens.shape, bf16),
        in_specs=[pl.BlockSpec(memory_space=pltpu.VMEM)] * 2,
        out_specs=pl.BlockSpec(memory_space=pltpu.HBM),
        scratch_shapes=[
            pltpu.VMEM(tokens.shape, bf16),
            pltpu.SemaphoreType.DMA((images * seq // chunk,)),
        ],
        compiler_params=pltpu.CompilerParams(vmem_limit_bytes=16 * 2**20),
    )(recv2, comb)


def solution(mesh):
    placed = (
        P(("expert", "tensor"), None, None),
        P(),
        P(),
        P("expert", None, "tensor"),
        P("expert", "tensor"),
        P("expert", "tensor", None),
        P("expert", None),
    )
    return jax.shard_map(
        functools.partial(local, mesh.shape["expert"], mesh.shape["tensor"], peers_of(mesh)),
        mesh=mesh,
        in_specs=placed,
        out_specs=P(("expert", "tensor"), None, None),
        check_vma=False,
    )
```

```python
import functools

import jax
import jax.numpy as jnp
from jax import lax
from jax.experimental import pallas as pl
from jax.experimental.pallas import tpu as pltpu
from jax.sharding import PartitionSpec as P

EPS = 1e-06
LOGICAL = pl.DeviceIdType.LOGICAL
NT = (((1,), (1,)), ((), ()))
UNROLL = 64
TILE = 128
SPLIT = 2


def peers_of(mesh):
    flat = list(mesh.devices.flat)
    where = [tuple(getattr(d, "coords", None) or (0, 0, 0)) for d in flat]
    away = [[abs(p - q) for p, q in zip(w, where[0])] for w in where]
    axis = max(range(len(where[0])), key=lambda a: max(w[a] for w in away))
    groups = {}
    for k in sorted(range(1, len(flat)), key=lambda k: (-sum(away[k]), -k)):
        groups.setdefault(away[k][axis], []).append(k)
    steps = []
    while any(groups.values()):
        for g in sorted(groups, reverse=True):
            steps += groups[g][:1]
            del groups[g][:1]
    first = [k for k in range(len(flat)) if where[k] == where[0]][:2]
    return steps, first


def kernel(
    experts, tensors, order,
    tokens_hbm, keys_hbm, scale_hbm, w_in_hbm, b_in_hbm, w_out_hbm, b_out_hbm,
    recv2, comb,
    tok, keys_ref, scale_ref, b_in_ref, b_out_ref, w_in, w_out, send1, recv1, hidden, send2,
    load_sem, send_sem1, recv_sem1, send_sem2, recv_sem2,
):
    images, seq, width = tok.shape
    slots = keys_ref.shape[0]
    rows = slots * images
    devices = experts * tensors
    e, t = lax.axis_index("expert"), lax.axis_index("tensor")
    me = e * tensors + t
    home = t * experts + e
    steps, first = order
    pow2 = devices & (devices - 1) == 0

    def each_peer(body, ahead=()):
        if pow2 and devices <= UNROLL:
            for j in ahead:
                pl.when(me != j)(functools.partial(body, j))
            for k in steps:
                j = me ^ k
                if ahead:
                    rest = functools.reduce(jnp.logical_and, [j != a for a in ahead])
                    pl.when(rest)(functools.partial(body, j))
                else:
                    body(j)
        else:
            @pl.loop(1, devices)
            def _(step):
                body(lax.rem(me + step, devices))

    barrier = pltpu.get_barrier_semaphore()
    each_peer(lambda j: pl.semaphore_signal(barrier, inc=1, device_id=j, device_id_type=LOGICAL))

    pairs = [
        (keys_hbm, keys_ref), (scale_hbm, scale_ref), (tokens_hbm, tok), (b_in_hbm, b_in_ref),
        (w_in_hbm.at[0], w_in), (b_out_hbm, b_out_ref), (w_out_hbm.at[0], w_out),
    ]
    loads = [pltpu.make_async_copy(src, dst, load_sem.at[i]) for i, (src, dst) in enumerate(pairs)]
    for load in loads:
        load.start()

    loads[0].wait()
    loads[1].wait()
    row_slot = lax.broadcasted_iota(jnp.int32, (rows, slots), 0) // images
    col_slot = lax.broadcasted_iota(jnp.int32, (rows, slots), 1)
    spread = jnp.where(row_slot == col_slot, 1.0, 0.0).astype(jnp.bfloat16)
    keys_t = jnp.dot(spread, keys_ref[...], preferred_element_type=jnp.float32)
    key_inv = lax.rsqrt(jnp.sum(keys_t * keys_t, axis=1, keepdims=True) + EPS)
    key_gain = key_inv * scale_ref[0]
    keys_b = keys_t.astype(jnp.bfloat16)

    loads[2].wait()
    flat = tok[...].reshape(images * seq, width)
    raw = lax.dot_general(keys_b, flat, NT, preferred_element_type=jnp.float32)
    part = jnp.zeros((images * seq, 128), jnp.float32)
    for c in range(width // 128):
        piece = flat[:, c * 128:(c + 1) * 128].astype(jnp.float32)
        part = part + piece * piece
    row_sq = lax.dot_general(
        jnp.ones((8, 128), jnp.float32), part, NT,
        precision=lax.Precision.HIGHEST, preferred_element_type=jnp.float32,
    )[0:1]
    logits = key_gain * lax.rsqrt(row_sq + EPS) * raw
    row_image = lax.broadcasted_iota(jnp.int32, logits.shape, 0) % images
    col_image = lax.broadcasted_iota(jnp.int32, logits.shape, 1) // seq
    expo = jnp.where(row_image == col_image, jnp.exp(logits), 0.0)
    dispatch = (expo / jnp.sum(expo, axis=1, keepdims=True)).astype(jnp.bfloat16)
    slot_in = jnp.dot(dispatch, flat, preferred_element_type=jnp.float32).astype(jnp.bfloat16)
    for s in range(slots):
        send1[s] = slot_in[s * images:(s + 1) * images]
    recv1[me] = send1[e]
    combine = expo / jnp.sum(expo, axis=0, keepdims=True)
    comb[...] = jnp.concatenate([combine] * tensors, axis=0).T.astype(jnp.bfloat16)

    pl.semaphore_wait(barrier, devices - 1)
    each_peer(lambda j: pltpu.make_async_remote_copy(
        src_ref=send1.at[j // tensors], dst_ref=recv1.at[me], send_sem=send_sem1, recv_sem=recv_sem1,
        device_id=j, device_id_type=LOGICAL,
    ).start())

    for load in loads[3:]:
        load.wait()
    others = recv1.at[pl.ds(0, devices - 1)]
    pltpu.make_async_copy(others, others, recv_sem1).wait()
    x = recv1[...].reshape(devices * images, width)
    half = w_in.shape[1]
    first_half = jnp.where(t == 0, 1.0, 0.0)
    for c in range(0, half, TILE):
        size = min(TILE, half - c)
        pre = jnp.dot(x, w_in[:, c:c + size], preferred_element_type=jnp.float32)
        pre = pre + b_in_ref[:, c:c + size].astype(jnp.float32)
        hidden[:, c:c + size] = jax.nn.gelu(pre).astype(jnp.bfloat16)
    h = hidden[...]
    part = width // 2 if width % 256 == 0 else width
    for c in range(0, width, part):
        y = jnp.dot(h, w_out[:, c:c + part], preferred_element_type=jnp.float32)
        y = y + b_out_ref[:, c:c + part].astype(jnp.float32) * first_half
        send2[:, :, c:c + part] = y.astype(jnp.bfloat16).reshape(devices, images, part)
    recv2[home] = send2[me]
    each_peer(lambda j: pltpu.make_async_remote_copy(
        src_ref=send2.at[j], dst_ref=recv2.at[home], send_sem=send_sem2, recv_sem=recv_sem2,
        device_id=j, device_id_type=LOGICAL,
    ).start(), first)

    pltpu.make_async_copy(others, others, send_sem1).wait()
    block = recv2.at[pl.ds(0, devices - 1)]
    pltpu.make_async_copy(block, block, send_sem2).wait()
    pltpu.make_async_copy(block, block, recv_sem2).wait()


def mix(chunk, recv2, comb, out_hbm, out, sem):
    images, seq, width = out_hbm.shape
    r = recv2[...].reshape(-1, width)
    for c in range(0, images * seq, chunk):
        at = c // seq, pl.ds(c % seq, chunk)
        for n in range(0, width, TILE):
            mixed = jnp.dot(comb[c:c + chunk], r[:, n:n + TILE], preferred_element_type=jnp.float32)
            out[at[0], at[1], n:n + TILE] = mixed.astype(jnp.bfloat16)
        pltpu.make_async_copy(out.at[at], out_hbm.at[at], sem).start()
    pltpu.make_async_copy(out, out_hbm, sem).wait()


def local(experts, tensors, order, tokens, slot_keys, logit_scale, w_in, b_in, w_out, b_out):
    images, seq, width = tokens.shape
    slots = slot_keys.shape[1]
    half = w_in.shape[2]
    devices = experts * tensors
    bf16 = jnp.bfloat16
    recv2, comb = pl.pallas_call(
        functools.partial(kernel, experts, tensors, order),
        out_shape=[
            pltpu.VMEM((devices, images, width), bf16),
            pltpu.VMEM((images * seq, tensors * slots * images), bf16),
        ],
        in_specs=[pl.BlockSpec(memory_space=pltpu.HBM)] * 7,
        out_specs=[pl.BlockSpec(memory_space=pltpu.VMEM)] * 2,
        scratch_shapes=[
            pltpu.VMEM((images, seq, width), bf16),
            pltpu.VMEM((slots, width), bf16),
            pltpu.SMEM((1,), jnp.float32),
            pltpu.VMEM((1, half), bf16),
            pltpu.VMEM((1, width), bf16),
            pltpu.VMEM((width, half), bf16),
            pltpu.VMEM((half, width), bf16),
            pltpu.VMEM((slots, images, width), bf16),
            pltpu.VMEM((devices, images, width), bf16),
            pltpu.VMEM((devices * images, half), bf16),
            pltpu.VMEM((devices, images, width), bf16),
            pltpu.SemaphoreType.DMA((7,)),
            pltpu.SemaphoreType.DMA,
            pltpu.SemaphoreType.DMA,
            pltpu.SemaphoreType.DMA,
            pltpu.SemaphoreType.DMA,
        ],
        compiler_params=pltpu.CompilerParams(collective_id=0, has_side_effects=True, vmem_limit_bytes=55 * 2**20),
    )(tokens, slot_keys.T, logit_scale.reshape(1), w_in, b_in, w_out, b_out)
    chunk = seq // SPLIT
    return pl.pallas_call(
        functools.partial(mix, chunk),
        out_shape=jax.ShapeDtypeStruct(tokens.shape, bf16),
        in_specs=[pl.BlockSpec(memory_space=pltpu.VMEM)] * 2,
        out_specs=pl.BlockSpec(memory_space=pltpu.HBM),
        scratch_shapes=[
            pltpu.VMEM(tokens.shape, bf16),
            pltpu.SemaphoreType.DMA,
        ],
        compiler_params=pltpu.CompilerParams(vmem_limit_bytes=16 * 2**20),
    )(recv2, comb)


def solution(mesh):
    placed = (
        P(("expert", "tensor"), None, None),
        P(),
        P(),
        P("expert", None, "tensor"),
        P("expert", "tensor"),
        P("expert", "tensor", None),
        P("expert", None),
    )
    return jax.shard_map(
        functools.partial(local, mesh.shape["expert"], mesh.shape["tensor"], peers_of(mesh)),
        mesh=mesh,
        in_specs=placed,
        out_specs=P(("expert", "tensor"), None, None),
        check_vma=False,
    )
```

```python
import functools

import jax
import jax.numpy as jnp
from jax import lax
from jax.experimental import pallas as pl
from jax.experimental.pallas import tpu as pltpu
from jax.sharding import PartitionSpec as P

EPS = 1e-06
LOGICAL = pl.DeviceIdType.LOGICAL
NT = (((1,), (1,)), ((), ()))
UNROLL = 64
TILE = 128
SPLIT = 2


def peers_of(mesh):
    flat = list(mesh.devices.flat)
    where = [tuple(getattr(d, "coords", None) or (0, 0, 0)) for d in flat]
    away = [[abs(p - q) for p, q in zip(w, where[0])] for w in where]
    axis = max(range(len(where[0])), key=lambda a: max(w[a] for w in away))
    groups = {}
    for k in sorted(range(1, len(flat)), key=lambda k: (-sum(away[k]), -k)):
        groups.setdefault(away[k][axis], []).append(k)
    steps = []
    while any(groups.values()):
        for g in sorted(groups, reverse=True):
            steps += groups[g][:1]
            del groups[g][:1]
    first = [k for k in range(len(flat)) if where[k] == where[0]][:2]
    hops = [sum(a) for a in away]
    last = sorted((k for k in range(len(flat)) if 0 < hops[k] >= max(hops) - 1), key=lambda k: (-hops[k], -away[k][axis], -k))
    return steps, first, last


def kernel(
    experts, tensors, order,
    tokens_hbm, keys_hbm, scale_hbm, w_in_hbm, b_in_hbm, w_out_hbm, b_out_hbm,
    recv2, comb,
    tok, keys_ref, scale_ref, b_in_ref, b_out_ref, w_in, w_out, send1, recv1, hidden, send2,
    load_sem, send_sem1, recv_sem1, send_sem2, recv_sem2,
):
    images, seq, width = tok.shape
    slots = keys_ref.shape[0]
    rows = slots * images
    devices = experts * tensors
    e, t = lax.axis_index("expert"), lax.axis_index("tensor")
    me = e * tensors + t
    home = t * experts + e
    steps, first, last = order
    pow2 = devices & (devices - 1) == 0

    def each_peer(body, ahead=()):
        if pow2 and devices <= UNROLL:
            for j in ahead:
                pl.when(me != j)(functools.partial(body, j))
            for k in steps:
                j = me ^ k
                if ahead:
                    rest = functools.reduce(jnp.logical_and, [j != a for a in ahead])
                    pl.when(rest)(functools.partial(body, j))
                else:
                    body(j)
        else:
            @pl.loop(1, devices)
            def _(step):
                body(lax.rem(me + step, devices))

    barrier = pltpu.get_barrier_semaphore()
    each_peer(lambda j: pl.semaphore_signal(barrier, inc=1, device_id=j, device_id_type=LOGICAL))

    pairs = [
        (keys_hbm, keys_ref), (scale_hbm, scale_ref), (tokens_hbm, tok), (b_in_hbm, b_in_ref),
        (w_in_hbm.at[0], w_in), (b_out_hbm, b_out_ref), (w_out_hbm.at[0], w_out),
    ]
    loads = [pltpu.make_async_copy(src, dst, load_sem.at[i]) for i, (src, dst) in enumerate(pairs)]
    for load in loads:
        load.start()

    loads[0].wait()
    loads[1].wait()
    row_slot = lax.broadcasted_iota(jnp.int32, (rows, slots), 0) // images
    col_slot = lax.broadcasted_iota(jnp.int32, (rows, slots), 1)
    spread = jnp.where(row_slot == col_slot, 1.0, 0.0).astype(jnp.bfloat16)
    keys_t = jnp.dot(spread, keys_ref[...], preferred_element_type=jnp.float32)
    key_inv = lax.rsqrt(jnp.sum(keys_t * keys_t, axis=1, keepdims=True) + EPS)
    key_gain = key_inv * scale_ref[0]
    keys_b = keys_t.astype(jnp.bfloat16)

    loads[2].wait()
    flat = tok[...].reshape(images * seq, width)
    raw = lax.dot_general(keys_b, flat, NT, preferred_element_type=jnp.float32)
    part = jnp.zeros((images * seq, 128), jnp.float32)
    for c in range(width // 128):
        piece = flat[:, c * 128:(c + 1) * 128].astype(jnp.float32)
        part = part + piece * piece
    row_sq = lax.dot_general(
        jnp.ones((8, 128), jnp.float32), part, NT,
        precision=lax.Precision.HIGHEST, preferred_element_type=jnp.float32,
    )[0:1]
    logits = key_gain * lax.rsqrt(row_sq + EPS) * raw
    row_image = lax.broadcasted_iota(jnp.int32, logits.shape, 0) % images
    col_image = lax.broadcasted_iota(jnp.int32, logits.shape, 1) // seq
    expo = jnp.where(row_image == col_image, jnp.exp(logits), 0.0)
    dispatch = (expo / jnp.sum(expo, axis=1, keepdims=True)).astype(jnp.bfloat16)
    slot_in = jnp.dot(dispatch, flat, preferred_element_type=jnp.float32).astype(jnp.bfloat16)
    for s in range(slots):
        send1[s] = slot_in[s * images:(s + 1) * images]
    recv1[me] = send1[e]
    combine = expo / jnp.sum(expo, axis=0, keepdims=True)
    comb[...] = jnp.concatenate([combine] * tensors, axis=0).T.astype(jnp.bfloat16)

    pl.semaphore_wait(barrier, devices - 1)
    each_peer(lambda j: pltpu.make_async_remote_copy(
        src_ref=send1.at[j // tensors], dst_ref=recv1.at[me], send_sem=send_sem1, recv_sem=recv_sem1,
        device_id=j, device_id_type=LOGICAL,
    ).start(), last)

    for load in loads[3:]:
        load.wait()
    others = recv1.at[pl.ds(0, devices - 1)]
    pltpu.make_async_copy(others, others, recv_sem1).wait()
    x = recv1[...].reshape(devices * images, width)
    half = w_in.shape[1]
    first_half = jnp.where(t == 0, 1.0, 0.0)
    for c in range(0, half, TILE):
        size = min(TILE, half - c)
        pre = jnp.dot(x, w_in[:, c:c + size], preferred_element_type=jnp.float32)
        pre = pre + b_in_ref[:, c:c + size].astype(jnp.float32)
        hidden[:, c:c + size] = jax.nn.gelu(pre).astype(jnp.bfloat16)
    h = hidden[...]
    part = width // 2 if width % 256 == 0 else width
    for c in range(0, width, part):
        y = jnp.dot(h, w_out[:, c:c + part], preferred_element_type=jnp.float32)
        y = y + b_out_ref[:, c:c + part].astype(jnp.float32) * first_half
        send2[:, :, c:c + part] = y.astype(jnp.bfloat16).reshape(devices, images, part)
    recv2[home] = send2[me]
    each_peer(lambda j: pltpu.make_async_remote_copy(
        src_ref=send2.at[j], dst_ref=recv2.at[home], send_sem=send_sem2, recv_sem=recv_sem2,
        device_id=j, device_id_type=LOGICAL,
    ).start(), first)

    pltpu.make_async_copy(others, others, send_sem1).wait()
    block = recv2.at[pl.ds(0, devices - 1)]
    pltpu.make_async_copy(block, block, send_sem2).wait()
    pltpu.make_async_copy(block, block, recv_sem2).wait()


def mix(chunk, recv2, comb, out_hbm, out, sem):
    images, seq, width = out_hbm.shape
    r = recv2[...].reshape(-1, width)
    for c in range(0, images * seq, chunk):
        at = c // seq, pl.ds(c % seq, chunk)
        for n in range(0, width, TILE):
            mixed = jnp.dot(comb[c:c + chunk], r[:, n:n + TILE], preferred_element_type=jnp.float32)
            out[at[0], at[1], n:n + TILE] = mixed.astype(jnp.bfloat16)
        pltpu.make_async_copy(out.at[at], out_hbm.at[at], sem).start()
    pltpu.make_async_copy(out, out_hbm, sem).wait()


def local(experts, tensors, order, tokens, slot_keys, logit_scale, w_in, b_in, w_out, b_out):
    images, seq, width = tokens.shape
    slots = slot_keys.shape[1]
    half = w_in.shape[2]
    devices = experts * tensors
    bf16 = jnp.bfloat16
    recv2, comb = pl.pallas_call(
        functools.partial(kernel, experts, tensors, order),
        out_shape=[
            pltpu.VMEM((devices, images, width), bf16),
            pltpu.VMEM((images * seq, tensors * slots * images), bf16),
        ],
        in_specs=[pl.BlockSpec(memory_space=pltpu.HBM)] * 7,
        out_specs=[pl.BlockSpec(memory_space=pltpu.VMEM)] * 2,
        scratch_shapes=[
            pltpu.VMEM((images, seq, width), bf16),
            pltpu.VMEM((slots, width), bf16),
            pltpu.SMEM((1,), jnp.float32),
            pltpu.VMEM((1, half), bf16),
            pltpu.VMEM((1, width), bf16),
            pltpu.VMEM((width, half), bf16),
            pltpu.VMEM((half, width), bf16),
            pltpu.VMEM((slots, images, width), bf16),
            pltpu.VMEM((devices, images, width), bf16),
            pltpu.VMEM((devices * images, half), bf16),
            pltpu.VMEM((devices, images, width), bf16),
            pltpu.SemaphoreType.DMA((7,)),
            pltpu.SemaphoreType.DMA,
            pltpu.SemaphoreType.DMA,
            pltpu.SemaphoreType.DMA,
            pltpu.SemaphoreType.DMA,
        ],
        compiler_params=pltpu.CompilerParams(collective_id=0, has_side_effects=True, vmem_limit_bytes=55 * 2**20),
    )(tokens, slot_keys.T, logit_scale.reshape(1), w_in, b_in, w_out, b_out)
    chunk = seq // SPLIT
    return pl.pallas_call(
        functools.partial(mix, chunk),
        out_shape=jax.ShapeDtypeStruct(tokens.shape, bf16),
        in_specs=[pl.BlockSpec(memory_space=pltpu.VMEM)] * 2,
        out_specs=pl.BlockSpec(memory_space=pltpu.HBM),
        scratch_shapes=[
            pltpu.VMEM(tokens.shape, bf16),
            pltpu.SemaphoreType.DMA,
        ],
        compiler_params=pltpu.CompilerParams(vmem_limit_bytes=16 * 2**20),
    )(recv2, comb)


def solution(mesh):
    placed = (
        P(("expert", "tensor"), None, None),
        P(),
        P(),
        P("expert", None, "tensor"),
        P("expert", "tensor"),
        P("expert", "tensor", None),
        P("expert", None),
    )
    return jax.shard_map(
        functools.partial(local, mesh.shape["expert"], mesh.shape["tensor"], peers_of(mesh)),
        mesh=mesh,
        in_specs=placed,
        out_specs=P(("expert", "tensor"), None, None),
        check_vma=False,
    )
```

```python
import functools

import jax
import jax.numpy as jnp
from jax import lax
from jax.experimental import pallas as pl
from jax.experimental.pallas import tpu as pltpu
from jax.sharding import PartitionSpec as P

EPS = 1e-06
LOGICAL = pl.DeviceIdType.LOGICAL
NT = (((1,), (1,)), ((), ()))
UNROLL = 64
TILE = 128
SPLIT = 2


def peers_of(mesh):
    flat = list(mesh.devices.flat)
    where = [tuple(getattr(d, "coords", None) or (0, 0, 0)) for d in flat]
    away = [[abs(p - q) for p, q in zip(w, where[0])] for w in where]
    axis = max(range(len(where[0])), key=lambda a: max(w[a] for w in away))
    groups = {}
    for k in sorted(range(1, len(flat)), key=lambda k: (-sum(away[k]), -k)):
        groups.setdefault(away[k][axis], []).append(k)
    steps = []
    while any(groups.values()):
        for g in sorted(groups, reverse=True):
            steps += groups[g][:1]
            del groups[g][:1]
    first = [k for k in range(len(flat)) if where[k] == where[0]][:2]
    hops = [sum(a) for a in away]
    last = sorted((k for k in range(len(flat)) if 0 < hops[k] >= max(hops) - 1), key=lambda k: (-hops[k], -away[k][axis], -k))
    return steps, first, last


def kernel(
    experts, tensors, order,
    tokens_hbm, keys_hbm, scale_hbm, w_in_hbm, b_in_hbm, w_out_hbm, b_out_hbm,
    recv2, comb,
    tok, keys_ref, scale_ref, b_in_ref, b_out_ref, w_in, w_out, send1, recv1, hidden, send2,
    load_sem, send_sem1, recv_sem1, send_sem2, recv_sem2,
):
    images, seq, width = tok.shape
    slots = keys_ref.shape[0]
    rows = slots * images
    devices = experts * tensors
    e, t = lax.axis_index("expert"), lax.axis_index("tensor")
    me = e * tensors + t
    home = t * experts + e
    steps, first, last = order
    pow2 = devices & (devices - 1) == 0

    def each_peer(body, ahead=()):
        if pow2 and devices <= UNROLL:
            for j in ahead:
                pl.when(me != j)(functools.partial(body, j))
            for k in steps:
                j = me ^ k
                if ahead:
                    rest = functools.reduce(jnp.logical_and, [j != a for a in ahead])
                    pl.when(rest)(functools.partial(body, j))
                else:
                    body(j)
        else:
            @pl.loop(1, devices)
            def _(step):
                body(lax.rem(me + step, devices))

    pairs = [
        (keys_hbm, keys_ref), (scale_hbm, scale_ref), (tokens_hbm, tok), (b_in_hbm, b_in_ref),
        (w_in_hbm.at[0], w_in), (b_out_hbm, b_out_ref), (w_out_hbm.at[0], w_out),
    ]
    loads = [pltpu.make_async_copy(src, dst, load_sem.at[i]) for i, (src, dst) in enumerate(pairs)]
    for load in loads[:3]:
        load.start()

    barrier = pltpu.get_barrier_semaphore()
    each_peer(lambda j: pl.semaphore_signal(barrier, inc=1, device_id=j, device_id_type=LOGICAL))

    loads[0].wait()
    loads[1].wait()
    row_slot = lax.broadcasted_iota(jnp.int32, (rows, slots), 0) // images
    col_slot = lax.broadcasted_iota(jnp.int32, (rows, slots), 1)
    spread = jnp.where(row_slot == col_slot, 1.0, 0.0).astype(jnp.bfloat16)
    keys_t = jnp.dot(spread, keys_ref[...], preferred_element_type=jnp.float32)
    key_inv = lax.rsqrt(jnp.sum(keys_t * keys_t, axis=1, keepdims=True) + EPS)
    key_gain = key_inv * scale_ref[0]
    keys_b = keys_t.astype(jnp.bfloat16)

    loads[2].wait()
    for load in loads[3:]:
        load.start()
    flat = tok[...].reshape(images * seq, width)
    raw = lax.dot_general(keys_b, flat, NT, preferred_element_type=jnp.float32)
    part = jnp.zeros((images * seq, 128), jnp.float32)
    for c in range(width // 128):
        piece = flat[:, c * 128:(c + 1) * 128].astype(jnp.float32)
        part = part + piece * piece
    row_sq = lax.dot_general(
        jnp.ones((8, 128), jnp.float32), part, NT,
        precision=lax.Precision.HIGHEST, preferred_element_type=jnp.float32,
    )[0:1]
    logits = key_gain * lax.rsqrt(row_sq + EPS) * raw
    row_image = lax.broadcasted_iota(jnp.int32, logits.shape, 0) % images
    col_image = lax.broadcasted_iota(jnp.int32, logits.shape, 1) // seq
    expo = jnp.where(row_image == col_image, jnp.exp(logits), 0.0)
    dispatch = (expo / jnp.sum(expo, axis=1, keepdims=True)).astype(jnp.bfloat16)
    slot_in = jnp.dot(dispatch, flat, preferred_element_type=jnp.float32).astype(jnp.bfloat16)
    for s in range(slots):
        send1[s] = slot_in[s * images:(s + 1) * images]
    recv1[me] = send1[e]
    combine = expo / jnp.sum(expo, axis=0, keepdims=True)
    comb[...] = jnp.concatenate([combine] * tensors, axis=0).T.astype(jnp.bfloat16)

    pl.semaphore_wait(barrier, devices - 1)
    each_peer(lambda j: pltpu.make_async_remote_copy(
        src_ref=send1.at[j // tensors], dst_ref=recv1.at[me], send_sem=send_sem1, recv_sem=recv_sem1,
        device_id=j, device_id_type=LOGICAL,
    ).start(), last)

    for load in loads[3:]:
        load.wait()
    others = recv1.at[pl.ds(0, devices - 1)]
    pltpu.make_async_copy(others, others, recv_sem1).wait()
    x = recv1[...].reshape(devices * images, width)
    half = w_in.shape[1]
    first_half = jnp.where(t == 0, 1.0, 0.0)
    for c in range(0, half, TILE):
        size = min(TILE, half - c)
        pre = jnp.dot(x, w_in[:, c:c + size], preferred_element_type=jnp.float32)
        pre = pre + b_in_ref[:, c:c + size].astype(jnp.float32)
        hidden[:, c:c + size] = jax.nn.gelu(pre).astype(jnp.bfloat16)
    h = hidden[...]
    part = width // 2 if width % 256 == 0 else width
    for c in range(0, width, part):
        y = jnp.dot(h, w_out[:, c:c + part], preferred_element_type=jnp.float32)
        y = y + b_out_ref[:, c:c + part].astype(jnp.float32) * first_half
        send2[:, :, c:c + part] = y.astype(jnp.bfloat16).reshape(devices, images, part)
    recv2[home] = send2[me]
    each_peer(lambda j: pltpu.make_async_remote_copy(
        src_ref=send2.at[j], dst_ref=recv2.at[home], send_sem=send_sem2, recv_sem=recv_sem2,
        device_id=j, device_id_type=LOGICAL,
    ).start(), first)

    pltpu.make_async_copy(others, others, send_sem1).wait()
    block = recv2.at[pl.ds(0, devices - 1)]
    pltpu.make_async_copy(block, block, send_sem2).wait()
    pltpu.make_async_copy(block, block, recv_sem2).wait()


def mix(chunk, recv2, comb, out_hbm, out, sem):
    images, seq, width = out_hbm.shape
    r = recv2[...].reshape(-1, width)
    for c in range(0, images * seq, chunk):
        at = c // seq, pl.ds(c % seq, chunk)
        for n in range(0, width, TILE):
            mixed = jnp.dot(comb[c:c + chunk], r[:, n:n + TILE], preferred_element_type=jnp.float32)
            out[at[0], at[1], n:n + TILE] = mixed.astype(jnp.bfloat16)
        pltpu.make_async_copy(out.at[at], out_hbm.at[at], sem).start()
    pltpu.make_async_copy(out, out_hbm, sem).wait()


def local(experts, tensors, order, tokens, slot_keys, logit_scale, w_in, b_in, w_out, b_out):
    images, seq, width = tokens.shape
    slots = slot_keys.shape[1]
    half = w_in.shape[2]
    devices = experts * tensors
    bf16 = jnp.bfloat16
    recv2, comb = pl.pallas_call(
        functools.partial(kernel, experts, tensors, order),
        out_shape=[
            pltpu.VMEM((devices, images, width), bf16),
            pltpu.VMEM((images * seq, tensors * slots * images), bf16),
        ],
        in_specs=[pl.BlockSpec(memory_space=pltpu.HBM)] * 7,
        out_specs=[pl.BlockSpec(memory_space=pltpu.VMEM)] * 2,
        scratch_shapes=[
            pltpu.VMEM((images, seq, width), bf16),
            pltpu.VMEM((slots, width), bf16),
            pltpu.SMEM((1,), jnp.float32),
            pltpu.VMEM((1, half), bf16),
            pltpu.VMEM((1, width), bf16),
            pltpu.VMEM((width, half), bf16),
            pltpu.VMEM((half, width), bf16),
            pltpu.VMEM((slots, images, width), bf16),
            pltpu.VMEM((devices, images, width), bf16),
            pltpu.VMEM((devices * images, half), bf16),
            pltpu.VMEM((devices, images, width), bf16),
            pltpu.SemaphoreType.DMA((7,)),
            pltpu.SemaphoreType.DMA,
            pltpu.SemaphoreType.DMA,
            pltpu.SemaphoreType.DMA,
            pltpu.SemaphoreType.DMA,
        ],
        compiler_params=pltpu.CompilerParams(collective_id=0, has_side_effects=True, vmem_limit_bytes=55 * 2**20),
    )(tokens, slot_keys.T, logit_scale.reshape(1), w_in, b_in, w_out, b_out)
    chunk = seq // SPLIT
    return pl.pallas_call(
        functools.partial(mix, chunk),
        out_shape=jax.ShapeDtypeStruct(tokens.shape, bf16),
        in_specs=[pl.BlockSpec(memory_space=pltpu.VMEM)] * 2,
        out_specs=pl.BlockSpec(memory_space=pltpu.HBM),
        scratch_shapes=[
            pltpu.VMEM(tokens.shape, bf16),
            pltpu.SemaphoreType.DMA,
        ],
        compiler_params=pltpu.CompilerParams(vmem_limit_bytes=16 * 2**20),
    )(recv2, comb)


def solution(mesh):
    placed = (
        P(("expert", "tensor"), None, None),
        P(),
        P(),
        P("expert", None, "tensor"),
        P("expert", "tensor"),
        P("expert", "tensor", None),
        P("expert", None),
    )
    return jax.shard_map(
        functools.partial(local, mesh.shape["expert"], mesh.shape["tensor"], peers_of(mesh)),
        mesh=mesh,
        in_specs=placed,
        out_specs=P(("expert", "tensor"), None, None),
        check_vma=False,
    )
```
